32 devices in a mesh: section: 4 (over y, x), dp: 8 (over z, core).
Axes of the slice: x: 2, y: 2, z: 4, core: 2. Of those that a mesh axis runs over, the one named last changes fastest.
Arguments:
- inputs: bfloat16 [8, 128, 16384], P(None, None, 'dp'), may hold values from -6 to 6
- cotangent: bfloat16 [4, 8, 128, 1024], P('section'), may hold values from -0.5 to 0.5
- norm_gain: bfloat16 [4, 16384], P('section', 'dp'), may hold values from 0.099609375 to 1.8984375
- value_weight: bfloat16 [4, 16384, 1024], P('section', 'dp'), may hold values from -0.046875 to 0.046875
- output_weight: bfloat16 [4, 1024, 16384], P('section', None, 'dp'), may hold values from -0.1875 to 0.1875
- left_old: float32 [4, 16, 1024, 1024], P('section', 'dp'), may hold values from -0.4 to 2.4, as said below
- right_old: float32 [4, 1024, 1024], P('section', 'dp'), may hold values from -0.4 to 2.4, as said below
Outputs:
- section_outputs: bfloat16 [4, 8, 128, 16384], P('section', None, None, 'dp')
- left_stats: float32 [4, 16, 1024, 1024], P('section', 'dp')
- right_stats: float32 [4, 1024, 1024], P('section', 'dp')
The draws below stay inside these ranges and needn't reach their ends.
Inputs may be any that keep to these rules, and one draw needn't show every extreme that they name: `left_old`: symmetric in its last two dimensions. `right_old`: symmetric in its last two dimensions.
All inputs are finite; a program needn't handle non-finite values.
Results may differ from the reference program's by a relative error of at most 0.015.
Values may be sent and summed in bfloat16 or wider, within the bound.
No kernel may reach another device: no remote copies, remote signals or barrier semaphores. Data moves between devices by JAX's collectives and lax.ppermute only.
A program may use at most 128 MiB of HBM per device.

```python
import jax
import jax.numpy as jnp
from jax import lax

D = 16384
KV = 1024
BLOCK = 1024
MICRO = 8
MB = 128
SECTIONS = 4
NB = 16
N_SECTION = 4


def symmetric(key, leading, order):
    key_noise, key_diag = jax.random.split(key)
    noise_part = jnp.clip(jax.random.normal(key_noise, leading + (order, order), jnp.float32), -4.0, 4.0) * 0.05
    diagonal = jax.random.uniform(key_diag, leading + (order,), jnp.float32, 0.5, 2.0)
    return noise_part + jnp.swapaxes(noise_part, -1, -2) + diagonal[..., None] * jnp.eye(order, dtype=jnp.float32)


def draw_left_old(key, part):
    return symmetric(jax.random.fold_in(key, 11), (SECTIONS, NB), BLOCK)


def draw_right_old(key, part):
    return symmetric(jax.random.fold_in(key, 23), (SECTIONS,), KV)


def block_scale(rng, dims, pieces, low, largest):
    factor_of = 1.0
    for dim, shards_of in pieces:
        heights = jax.random.uniform(jax.random.fold_in(jax.random.fold_in(rng, 6), dim), (shards_of,), jnp.float32, low / len(pieces), largest / len(pieces))
        factor_of = factor_of * jnp.repeat(jnp.exp(heights), dims[dim] // shards_of).reshape((-1,) + (1,) * (len(dims) - 1 - dim))
    return factor_of


def normal_values(stream_key, extent, spread, reach, cuts=(), kind=jnp.bfloat16):
    array = jax.random.normal(stream_key, extent, jnp.float32) * spread
    if len(cuts) > 0:
        array = block_scale(stream_key, extent, cuts, -0.22, 0.18) * array
    return jnp.clip(array, min=-reach, max=reach).astype(kind)


def setup_inputs(seed: int = 0) -> dict:
    keys = jax.random.split(jax.random.key(seed), 8)
    return {
        "inputs": normal_values(keys[0], (MICRO, MB, D), 1.0, 6.0, ((2, 8),)),
        "cotangent": normal_values(keys[1], (SECTIONS, MICRO, MB, KV), 0.08, 0.5, ((0, 4),)),
        "norm_gain": jnp.clip(1.0 + 0.18 * jax.random.normal(keys[2], (SECTIONS, D), jnp.float32), 0.099609375, 1.8984375).astype(jnp.bfloat16),
        "value_weight": normal_values(keys[3], (SECTIONS, D, KV), D ** -0.5, 0.046875, ((0, 4), (1, 8))),
        "output_weight": normal_values(keys[4], (SECTIONS, KV, D), KV ** -0.5, 0.1875, ((0, 4), (2, 8))),
        "left_old": draw_left_old(jax.random.fold_in(keys[7], 71), 0),
        "right_old": draw_right_old(jax.random.fold_in(keys[7], 71), 0),
    }


def reference(inputs, cotangent, norm_gain, value_weight, output_weight, left_old, right_old):
    micro_count, batch_rows, model_width = inputs.shape
    hidden_in = inputs.reshape(micro_count * batch_rows, model_width)
    outputs_all = []
    lefts_all = []
    rights_all = []
    for layer_index in range(N_SECTION):
        floats = hidden_in.astype(jnp.float32)
        scaled_in = (floats * norm_gain[layer_index].astype(jnp.float32)).astype(jnp.bfloat16)
        inv_rms = lax.rsqrt(lax.optimization_barrier(jnp.mean(floats * floats, axis=1)) + 0.25)
        products = jnp.dot(scaled_in, value_weight[layer_index], preferred_element_type=jnp.float32)
        values = (inv_rms[:, None] * products).astype(jnp.bfloat16)
        hidden_in = (floats + jnp.dot(values, output_weight[layer_index], preferred_element_type=jnp.float32)).astype(jnp.bfloat16)
        cotan_rows = cotangent[layer_index].reshape(micro_count * batch_rows, KV).astype(jnp.float32)
        weighted = (inv_rms[:, None] * cotan_rows).astype(jnp.bfloat16)
        gradient = jnp.dot(scaled_in.T, weighted, preferred_element_type=jnp.float32).astype(jnp.bfloat16)
        blocks = gradient.reshape(NB, BLOCK, KV).astype(jnp.float32)
        left_new = left_old[layer_index] + jnp.einsum('bik,bjk->bij', blocks, blocks, precision=lax.Precision.HIGHEST) / BLOCK
        right_new = right_old[layer_index] + jnp.dot(gradient.T, gradient, preferred_element_type=jnp.float32) / D
        outputs_all.append(hidden_in.reshape(micro_count, batch_rows, model_width))
        lefts_all.append(left_new)
        rights_all.append(right_new)
    return (jnp.stack(outputs_all), jnp.stack(lefts_all), jnp.stack(rights_all))
```

```python
import functools

import jax
import jax.numpy as jnp
from jax import lax
from jax.experimental import pallas as pl
from jax.experimental.pallas import tpu as pltpu
from jax.sharding import PartitionSpec as P


BLOCK = 1024
LANES = 128
LAG = 3
TILE = 256


def swap(value, axis, mask):
    count = lax.axis_size(axis)
    return lax.ppermute(value, axis, [(i, i ^ mask) for i in range(count)])


def passed_along(value, axis):
    count = lax.axis_size(axis)
    return lax.ppermute(value, axis, [(i, i + 1) for i in range(count - 1)])


def put_pair(ref, total):
    high = total.astype(jnp.bfloat16)
    low = (total - high.astype(jnp.float32)).astype(jnp.bfloat16)
    rows = total.shape[0]
    lane = lax.broadcasted_iota(jnp.int32, (rows, LANES), 1)
    high = jnp.broadcast_to(high.astype(jnp.float32), (rows, LANES))
    low = jnp.broadcast_to(low.astype(jnp.float32), (rows, LANES))
    ref[...] = jnp.where(lane < LANES // 2, high, low).astype(jnp.bfloat16)


def get_pair(block):
    wide = block.astype(jnp.float32)
    return wide[:, :1] + wide[:, LANES // 2 : LANES // 2 + 1]


def project_kernel(first, where_ref, entering_ref, moved_ref, gain_ref, weight_ref, *rest):
    keep_ref, send_ref = rest[-2:]
    rows, wide = keep_ref.shape
    half = wide - LANES
    start = entering_ref[first * rows : (first + 1) * rows, :]
    hidden = jnp.where(where_ref[0] == 0, start, moved_ref[...]).astype(jnp.float32)
    scaled = (hidden * gain_ref[...].astype(jnp.float32)).astype(jnp.bfloat16)
    square = jnp.sum(hidden * hidden, axis=1, keepdims=True)
    put_pair(keep_ref.at[:, half:], square)
    put_pair(send_ref.at[:, half:], square)
    own = pl.multiple_of(where_ref[1] * half, LANES)
    theirs = pl.multiple_of((1 - where_ref[1]) * half, LANES)
    tile = min(TILE, half)
    for ref, first_col in ((send_ref, theirs), (keep_ref, own)):

        @pl.loop(0, half // tile)
        def _(index):
            at = pl.multiple_of(index * tile, LANES)
            ref[:, pl.ds(at, tile)] = jnp.dot(
                scaled, weight_ref[:, pl.ds(first_col + at, tile)], preferred_element_type=jnp.float32
            ).astype(jnp.bfloat16)


def join_kernel(mine_ref, other_ref, out_ref):
    half = out_ref.shape[1] - LANES
    out_ref[:, :half] = (
        mine_ref[:, :half].astype(jnp.float32) + other_ref[:, :half].astype(jnp.float32)
    ).astype(jnp.bfloat16)
    put_pair(out_ref.at[:, half:], get_pair(mine_ref[:, half:]) + get_pair(other_ref[:, half:]))


def value_kernel(pairs, model_width, *refs):
    parts, out_ref = refs[:pairs], refs[-1]
    half = out_ref.shape[1] - LANES
    total = parts[0][:, :half].astype(jnp.float32)
    square = get_pair(parts[0][:, half:])
    for part in parts[1:]:
        total += part[:, :half].astype(jnp.float32)
        square += get_pair(part[:, half:])
    inv_rms = lax.rsqrt(square / model_width + 0.25)
    out_ref[:, :half] = (inv_rms * total).astype(jnp.bfloat16)
    put_pair(out_ref.at[:, half:], inv_rms)


def output_kernel(first, slot, count, where_ref, mine_ref, other_ref, entering_ref, moved_ref, gain_ref, weight_ref, cotan_ref, *rest):
    result_ref, out_ref, scaled_ref, weighted_ref, values, cotan, scaled, weighted, sems = rest[-9:]
    rows, wide = mine_ref.shape
    half = wide - LANES
    at = pl.ds(pl.multiple_of(jnp.clip(slot - LAG * where_ref[0], 0, count - 1) * rows, 16), rows)
    fetch = pltpu.make_async_copy(cotan_ref.at[at, :], cotan, sems.at[0])
    fetch.start()
    values[:, pl.ds(pl.multiple_of(where_ref[1] * half, LANES), half)] = mine_ref[:, :half]
    values[:, pl.ds(pl.multiple_of((1 - where_ref[1]) * half, LANES), half)] = other_ref[:, :half]
    held_rows = pl.ds(first * rows, rows)
    tile = min(2 * TILE, result_ref.shape[1])

    @pl.loop(0, result_ref.shape[1] // tile)
    def _(index):
        part = pl.ds(pl.multiple_of(index * tile, LANES), tile)
        hidden = jnp.where(where_ref[0] == 0, entering_ref[held_rows, part], moved_ref[:, part]).astype(jnp.float32)
        scaled[:, part] = (hidden * gain_ref[:, part].astype(jnp.float32)).astype(jnp.bfloat16)
        result_ref[:, part] = (
            hidden + jnp.dot(values[...], weight_ref[:, part], preferred_element_type=jnp.float32)
        ).astype(jnp.bfloat16)

    store_scaled = pltpu.make_async_copy(scaled, scaled_ref.at[at, :], sems.at[1])
    store_scaled.start()
    store_out = pltpu.make_async_copy(result_ref, out_ref.at[at, :], sems.at[2])
    store_out.start()
    fetch.wait()
    weighted[...] = (get_pair(mine_ref[:, half:]) * cotan[...].astype(jnp.float32)).astype(jnp.bfloat16)
    store_weighted = pltpu.make_async_copy(weighted, weighted_ref.at[at, :], sems.at[3])
    store_weighted.start()
    store_scaled.wait()
    store_out.wait()
    store_weighted.wait()


def local_call(kernel, outs, operands, remote=(), aliases=None, scratch=(), limit=16):
    vmem = pl.BlockSpec(memory_space=pltpu.VMEM)
    hbm = pl.BlockSpec(memory_space=pl.ANY)
    scalars = 1 if operands[0].dtype == jnp.int32 else 0
    held = [pltpu.with_memory_space_constraint(x, pltpu.VMEM) for x in operands[scalars:]]
    near = [o for o in outs if not isinstance(o, tuple)]
    far = [pltpu.HBM(*o) for o in outs if isinstance(o, tuple)]
    return pl.pallas_call(
        kernel,
        out_shape=tuple([pltpu.VMEM(o.shape, o.dtype) for o in near] + far),
        in_specs=[pl.BlockSpec(memory_space=pltpu.SMEM)] * scalars + [vmem] * len(held) + [hbm] * len(remote),
        out_specs=(vmem,) * len(near) + (hbm,) * len(far),
        scratch_shapes=scratch,
        input_output_aliases=aliases or {},
        compiler_params=pltpu.CompilerParams(vmem_limit_bytes=limit << 20),
    )(*operands[:scalars], *held, *remote)


def on_device(inputs, cotangent, norm_gain, value_weight, output_weight, left_old, right_old):
    sections = lax.axis_size("section")
    dp_count = lax.axis_size("dp")
    section_index = lax.axis_index("section")
    owner_index = lax.axis_index("dp")
    core_index = owner_index % 2
    pair_index = owner_index // 2
    pairs = dp_count // 2
    micro_count, rows, cols = inputs.shape
    width_kv = value_weight.shape[2]
    half = width_kv // 2
    wide = half + LANES
    tokens = micro_count * rows
    entering = inputs.reshape(tokens, cols)
    cotan = cotangent.reshape(tokens, width_kv)
    w_value = value_weight[0]
    w_output = output_weight[0]
    where_am_i = jnp.stack([section_index, core_index]).astype(jnp.int32)
    count = micro_count
    slots = count + LAG * (sections - 1)
    bf16 = lambda *shape: jax.ShapeDtypeStruct(shape, jnp.bfloat16)
    message = bf16(rows, wide)

    def project(slot, moved, behind):
        first = min(slot, count - 1)
        return local_call(
            functools.partial(project_kernel, first),
            (message, message),
            (where_am_i, entering, moved, norm_gain, w_value) + (() if behind is None else (behind,)),
        )

    def emit(slot, mine, other, moved, buffers):
        first = min(slot, count - 1)
        operands = (where_am_i, mine, other, entering, moved, norm_gain, w_output)
        aliases = {len(operands) + 1 + i: 1 + i for i in range(len(buffers))}
        big = ((tokens, cols), jnp.bfloat16)
        narrow = ((tokens, width_kv), jnp.bfloat16)
        return local_call(
            functools.partial(output_kernel, first, slot, count),
            (bf16(rows, cols), big, big, narrow),
            operands,
            (cotan,) + buffers,
            aliases,
            (
                pltpu.VMEM((rows, width_kv), jnp.bfloat16),
                pltpu.VMEM((rows, width_kv), jnp.bfloat16),
                pltpu.VMEM((rows, cols), jnp.bfloat16),
                pltpu.VMEM((rows, width_kv), jnp.bfloat16),
                pltpu.SemaphoreType.DMA((4,)),
            ),
        )

    buffers = ()
    moved = [jnp.zeros((rows, cols), jnp.bfloat16)] * LAG
    waiting = None
    behind = None
    for slot in range(slots + 1):
        if slot < slots:
            keep, send = project(slot, moved[slot], behind)
            (pair_sum,) = local_call(join_kernel, (message,), (keep, swap(send, "dp", 1)))
            entered = [pair_sum] + [swap(pair_sum, "dp", 2 * mask) for mask in range(1, pairs)]
        if slot > 0:
            (mine,) = local_call(
                functools.partial(value_kernel, pairs, cols * dp_count), (message,), waiting + [pair_sum]
            )
            behind, *buffers = emit(slot - 1, mine, swap(mine, "dp", 1), moved[slot - 1], tuple(buffers))
            if slot - 1 + LAG < slots:
                moved.append(passed_along(behind, "section"))
        waiting = entered

    outputs_buf, scaled_all, weighted_all = buffers
    contract_rows = (((0,), (0,)), ((), ()))
    gradient = lax.dot_general(
        scaled_all, weighted_all, contract_rows, preferred_element_type=jnp.float32
    ).astype(jnp.bfloat16)

    share = width_kv // dp_count
    right_part = (
        lax.dot_general(gradient, gradient, contract_rows, preferred_element_type=jnp.float32)
        .astype(jnp.bfloat16)
        .reshape(pairs, 2, share, width_kv)
    )
    theirs = lax.dynamic_index_in_dim(right_part, 1 - core_index, 1, keepdims=False)
    ours = lax.dynamic_index_in_dim(right_part, core_index, 1, keepdims=False)
    from_core = swap(theirs, "dp", 1)
    pair_right = ours.astype(jnp.float32) + from_core.astype(jnp.float32)

    def piece(mask):
        return lax.dynamic_index_in_dim(pair_right, pair_index ^ mask, 0, keepdims=False)

    right_rows = piece(0)
    for mask in range(1, pairs):
        right_rows = right_rows + swap(piece(mask).astype(jnp.bfloat16), "dp", 2 * mask).astype(jnp.float32)
    right_new = right_old[0] + right_rows / (cols * dp_count)

    blocks = gradient.reshape(cols // BLOCK, BLOCK, width_kv)
    left_new = (
        left_old[0]
        + jnp.einsum("bik,bjk->bij", blocks, blocks, preferred_element_type=jnp.float32) / BLOCK
    )
    return (outputs_buf.reshape(1, micro_count, rows, cols), left_new[None], right_new[None])


def solution(mesh):
    placed = (
        P(None, None, "dp"),
        P("section", None, None, None),
        P("section", "dp"),
        P("section", "dp", None),
        P("section", None, "dp"),
        P("section", "dp", None, None),
        P("section", "dp", None),
    )
    return jax.shard_map(
        on_device,
        mesh=mesh,
        in_specs=placed,
        out_specs=(
            P("section", None, None, "dp"),
            P("section", "dp", None, None),
            P("section", "dp", None),
        ),
        check_vma=False,
    )
```

```python
import functools

import jax
import jax.numpy as jnp
from jax import lax
from jax.experimental import pallas as pl
from jax.experimental.pallas import tpu as pltpu
from jax.sharding import PartitionSpec as P


BLOCK = 1024
LANES = 128
LAG = 3
EXTRA = 8


def swap(value, axis, mask):
    count = lax.axis_size(axis)
    return lax.ppermute(value, axis, [(i, i ^ mask) for i in range(count)])


def passed_along(value, axis):
    count = lax.axis_size(axis)
    return lax.ppermute(value, axis, [(i, i + 1) for i in range(count - 1)])


def put_pair(ref, total):
    high = total.astype(jnp.bfloat16)
    low = (total - high.astype(jnp.float32)).astype(jnp.bfloat16)
    rows = total.shape[0]
    lane = lax.broadcasted_iota(jnp.int32, (rows, LANES), 1)
    high = jnp.broadcast_to(high.astype(jnp.float32), (rows, LANES))
    low = jnp.broadcast_to(low.astype(jnp.float32), (rows, LANES))
    ref[...] = jnp.where(lane < LANES // 2, high, low).astype(jnp.bfloat16)


def get_pair(block):
    wide = block.astype(jnp.float32)
    return wide[:, :1] + wide[:, LANES // 2 : LANES // 2 + 1]


def project_kernel(count, state_ref, entering_ref, moved_ref, gain_ref, weight_ref, *rest):
    keep_ref, send_ref, next_ref = rest[-3:]
    rows, wide = keep_ref.shape
    half = wide - LANES
    next_ref[0] = state_ref[0]
    next_ref[1] = state_ref[1]
    next_ref[2] = state_ref[2] + 1
    next_ref[3] = state_ref[3]
    hidden = chosen(count, rows, state_ref, entering_ref, moved_ref, slice(None))
    scaled = (hidden * gain_ref[...].astype(jnp.float32)).astype(jnp.bfloat16)
    square = jnp.sum(hidden * hidden, axis=1, keepdims=True)
    put_pair(keep_ref.at[:, half:], square)
    put_pair(send_ref.at[:, half:], square)
    own = pl.multiple_of(state_ref[1] * half, LANES)
    theirs = pl.multiple_of((1 - state_ref[1]) * half, LANES)
    for ref, first_col in ((send_ref, theirs), (keep_ref, own)):
        ref[:, :half] = jnp.dot(
            scaled, weight_ref[:, pl.ds(first_col, half)], preferred_element_type=jnp.float32
        ).astype(jnp.bfloat16)


def chosen(count, rows, state_ref, entering_ref, moved_ref, part):
    first = pl.multiple_of(jnp.minimum(state_ref[2], count - 1) * rows, 16)
    entered = entering_ref[pl.ds(first, rows), part]
    return jnp.where(state_ref[0] == 0, entered, moved_ref[:, part]).astype(jnp.float32)


def place(count, rows, state_ref):
    return pl.ds(pl.multiple_of(jnp.clip(state_ref[2] - LAG * state_ref[0], 0, count - 1) * rows, 16), rows)


def join_kernel(mine_ref, other_ref, out_ref):
    rows = mine_ref.shape[0]
    half = out_ref.shape[1]
    out_ref[:rows, :] = (
        mine_ref[:, :half].astype(jnp.float32) + other_ref[:, :half].astype(jnp.float32)
    ).astype(jnp.bfloat16)
    total = get_pair(mine_ref[:, half:]) + get_pair(other_ref[:, half:])
    along = jnp.transpose(jnp.broadcast_to(total, (rows, LANES)))[:EXTRA, :]
    high = along.astype(jnp.bfloat16)
    out_ref[rows:, :] = jnp.zeros((EXTRA, half), jnp.bfloat16)
    out_ref[rows:, :rows] = high
    out_ref[rows:, rows : 2 * rows] = (along - high.astype(jnp.float32)).astype(jnp.bfloat16)


def value_kernel(pairs, model_width, *refs):
    parts, out_ref = refs[:pairs], refs[-1]
    rows = out_ref.shape[0]
    half = out_ref.shape[1] - LANES
    total = jnp.zeros((rows, half), jnp.float32)
    square = jnp.zeros((EXTRA, rows), jnp.float32)
    for part in parts:
        total += part[:rows, :].astype(jnp.float32)
        square += part[rows:, :rows].astype(jnp.float32) + part[rows:, rows : 2 * rows].astype(jnp.float32)
    inv_rms = lax.rsqrt(square / model_width + 0.25)
    inv_rms = jnp.transpose(jnp.broadcast_to(inv_rms[:1, :], (LANES, rows)))[:, :1]
    out_ref[:, :half] = (inv_rms * total).astype(jnp.bfloat16)
    put_pair(out_ref.at[:, half:], inv_rms)


def gather_values(state_ref, mine_ref, other_ref, values):
    half = mine_ref.shape[1] - LANES
    values[:, pl.ds(pl.multiple_of(state_ref[1] * half, LANES), half)] = mine_ref[:, :half]
    values[:, pl.ds(pl.multiple_of((1 - state_ref[1]) * half, LANES), half)] = other_ref[:, :half]


def keep_operands(count, state_ref, mine_ref, hidden, gain_ref, cotan_ref, scaled_ref, weighted_ref):
    rows, wide = mine_ref.shape
    at = place(count, rows, state_ref)
    scaled_ref[at, :] = (hidden * gain_ref[...].astype(jnp.float32)).astype(jnp.bfloat16)
    inv_rms = get_pair(mine_ref[:, wide - LANES :])
    weighted_ref[at, :] = (inv_rms * cotan_ref[at, :].astype(jnp.float32)).astype(jnp.bfloat16)


def output_kernel(count, state_ref, mine_ref, other_ref, entering_ref, moved_ref, weight_ref, gain_ref, cotan_ref, *rest):
    result_ref, out_ref, scaled_ref, weighted_ref, values = rest[-5:]
    rows = mine_ref.shape[0]
    gather_values(state_ref, mine_ref, other_ref, values)
    at = place(count, rows, state_ref)
    inv_rms = get_pair(mine_ref[:, mine_ref.shape[1] - LANES :])
    weighted_ref[at, :] = (inv_rms * cotan_ref[at, :].astype(jnp.float32)).astype(jnp.bfloat16)
    hidden = chosen(count, rows, state_ref, entering_ref, moved_ref, slice(None))
    scaled_ref[at, :] = (hidden * gain_ref[...].astype(jnp.float32)).astype(jnp.bfloat16)
    result = (hidden + jnp.dot(values[...], weight_ref[...], preferred_element_type=jnp.float32)).astype(jnp.bfloat16)
    result_ref[...] = result
    out_ref[at, :] = result


def operands_kernel(count, state_ref, mine_ref, entering_ref, moved_ref, gain_ref, cotan_ref, *rest):
    scaled_ref, weighted_ref = rest[-2:]
    hidden = chosen(count, mine_ref.shape[0], state_ref, entering_ref, moved_ref, slice(None))
    keep_operands(count, state_ref, mine_ref, hidden, gain_ref, cotan_ref, scaled_ref, weighted_ref)


def late_output_kernel(count, state_ref, mine_ref, other_ref, entering_ref, moved_ref, weight_ref, held_ref, out_ref, values):
    rows = mine_ref.shape[0]
    gather_values(state_ref, mine_ref, other_ref, values)
    hidden = chosen(count, rows, state_ref, entering_ref, moved_ref, slice(None))
    out_ref[place(count, rows, state_ref), :] = (
        hidden + jnp.dot(values[...], weight_ref[...], preferred_element_type=jnp.float32)
    ).astype(jnp.bfloat16)


CONTRACT_ROWS = (((0,), (0,)), ((), ()))


def first_gradient_kernel(rows, scaled_ref, weighted_ref, out_ref):
    cols, _ = out_ref.shape
    before = weighted_ref.shape[0] - rows
    tile = min(512, cols)

    @pl.loop(0, cols // tile)
    def _(index):
        at = pl.ds(pl.multiple_of(index * tile, tile), tile)
        out_ref[at, :] = lax.dot_general(
            scaled_ref[:before, at], weighted_ref[:before, :], CONTRACT_ROWS, preferred_element_type=jnp.float32
        )


def gradient_kernel(count, state_ref, mine_ref, entering_ref, moved_ref, gain_ref, cotan_ref, sum_ref, out_ref, weighted):
    rows, wide = mine_ref.shape
    cols = out_ref.shape[0]
    tile = min(512, cols)
    inv_rms = get_pair(mine_ref[:, wide - LANES :])
    weighted[...] = (inv_rms * cotan_ref[...].astype(jnp.float32)).astype(jnp.bfloat16)

    @pl.loop(0, cols // tile)
    def _(index):
        at = pl.ds(pl.multiple_of(index * tile, tile), tile)
        hidden = chosen(count, rows, state_ref, entering_ref, moved_ref, at)
        scaled = (hidden * gain_ref[:, at].astype(jnp.float32)).astype(jnp.bfloat16)
        out_ref[at, :] = (
            sum_ref[at, :]
            + lax.dot_general(scaled, weighted[...], CONTRACT_ROWS, preferred_element_type=jnp.float32)
        ).astype(jnp.bfloat16)


def right_kernel(masks, state_ref, gradient_ref, *rest):
    ours_ref, theirs_ref, block = rest[-3:]
    _, share, _ = ours_ref.shape

    @pl.loop(0, len(masks))
    def _(index):
        pair = state_ref[3] ^ (masks[0] - index)
        at = pl.ds(pl.multiple_of(pair * 2 * share, 2 * share), 2 * share)
        block[...] = lax.dot_general(
            gradient_ref[:, at], gradient_ref[...], CONTRACT_ROWS, preferred_element_type=jnp.float32
        )
        core = state_ref[1]
        ours_ref[index] = block[pl.ds(pl.multiple_of(core * share, share), share), :].astype(jnp.bfloat16)
        theirs_ref[index] = block[pl.ds(pl.multiple_of((1 - core) * share, share), share), :].astype(jnp.bfloat16)


def right_pieces_kernel(ours_ref, came_ref, *piece_refs):
    for index, ref in enumerate(piece_refs):
        ref[...] = (ours_ref[index].astype(jnp.float32) + came_ref[index].astype(jnp.float32)).astype(ref.dtype)


def left_kernel(gradient_ref, held_ref, old_ref, out_ref, stored_ref, sem):
    block, part = pl.program_id(0), pl.program_id(1)
    height, order = old_ref.shape[1:]
    store = pltpu.make_async_copy(held_ref, stored_ref, sem)

    @pl.when((block == 0) & (part == 0))
    def _():
        store.start()

    whole = pl.ds(pl.multiple_of(block * order, order), order)
    rows = pl.ds(pl.multiple_of(block * order + part * height, height), height)
    product = lax.dot_general(
        gradient_ref[rows, :], gradient_ref[whole, :], (((1,), (1,)), ((), ())), preferred_element_type=jnp.float32
    )
    out_ref[0] = old_ref[0] + product / order

    @pl.when((block == pl.num_programs(0) - 1) & (part == pl.num_programs(1) - 1))
    def _():
        store.wait()


def local_call(kernel, outs, operands, remote=(), aliases=None, scratch=(), limit=16):
    def space(x):
        return pltpu.SMEM if x.dtype == jnp.int32 else pltpu.VMEM

    far = [o for o in outs if isinstance(o, tuple)]
    near = [o for o in outs if not isinstance(o, tuple)]
    hbm = pl.BlockSpec(memory_space=pl.ANY)
    return pl.pallas_call(
        kernel,
        out_shape=tuple([space(o)(o.shape, o.dtype) for o in near] + [pltpu.HBM(*o) for o in far]),
        in_specs=[pl.BlockSpec(memory_space=space(x)) for x in operands] + [hbm] * len(remote),
        out_specs=tuple([pl.BlockSpec(memory_space=space(o)) for o in near] + [hbm] * len(far)),
        scratch_shapes=scratch,
        input_output_aliases=aliases or {},
        compiler_params=pltpu.CompilerParams(vmem_limit_bytes=limit << 20),
    )(*[pltpu.with_memory_space_constraint(x, space(x)) for x in operands], *remote)


def on_device(inputs, cotangent, norm_gain, value_weight, output_weight, left_old, right_old):
    sections = lax.axis_size("section")
    dp_count = lax.axis_size("dp")
    section_index = lax.axis_index("section")
    owner_index = lax.axis_index("dp")
    core_index = owner_index % 2
    pair_index = owner_index // 2
    pairs = dp_count // 2
    micro_count, rows, cols = inputs.shape
    width_kv = value_weight.shape[2]
    half = width_kv // 2
    wide = half + LANES
    tokens = micro_count * rows
    entering = inputs.reshape(tokens, cols)
    cotan = cotangent.reshape(tokens, width_kv)
    w_value = value_weight[0]
    w_output = output_weight[0]
    state = jnp.stack([section_index, core_index, jnp.zeros_like(core_index), pair_index]).astype(jnp.int32)
    count = micro_count
    slots = count + LAG * (sections - 1)
    bf16 = lambda *shape: jax.ShapeDtypeStruct(shape, jnp.bfloat16)
    message = bf16(rows, wide)

    def project(state, moved, behind):
        alone = behind is None
        return local_call(
            functools.partial(project_kernel, 1 if alone else count),
            (message, message, jax.ShapeDtypeStruct(state.shape, jnp.int32)),
            (state, inputs[0] if alone else entering, moved, norm_gain, w_value) + (() if behind is None else (behind,)),
        )

    stored = (bf16(tokens, cols), bf16(tokens, cols), bf16(tokens, width_kv))
    values = (pltpu.VMEM((rows, width_kv), jnp.bfloat16),)

    def emit(state, mine, other, moved, buffers):
        operands = (state, mine, other, entering, moved, w_output, norm_gain, cotan)
        return local_call(
            functools.partial(output_kernel, count),
            (bf16(rows, cols),) + stored,
            operands + buffers,
            (),
            {len(operands) + i: 1 + i for i in range(len(buffers))},
            values,
        )

    def late_emit(state, mine, other, moved, held):
        operands = (state, mine, other, entering, moved, w_output)
        (held,) = local_call(
            functools.partial(late_output_kernel, count), stored[:1], operands + (held,), (), {len(operands): 0}, values
        )
        return held

    buffers = ()
    moved = [jnp.zeros((rows, cols), jnp.bfloat16)] * LAG
    states = [state]
    waiting = None
    behind = None
    for slot in range(slots):
        keep, send, state = project(states[slot], moved[slot], behind if slot else None)
        states.append(state)
        (pair_sum,) = local_call(join_kernel, (bf16(rows + EXTRA, half),), (keep, swap(send, "dp", 1)))
        entered = [pair_sum]
        for mask in range(pairs - 1, 0, -1):
            entered.append(swap(pair_sum, "dp", 2 * mask))
        if slot == 0:
            behind = pair_sum
        if slot > 0:
            (mine,) = local_call(
                functools.partial(value_kernel, pairs, cols * dp_count), (message,), waiting + [pair_sum]
            )
            if slot < slots - 1:
                behind, *buffers = emit(states[slot - 1], mine, swap(mine, "dp", 1), moved[slot - 1], tuple(buffers))
            if slot - 1 + LAG < slots:
                moved.append(passed_along(behind, "section"))
        waiting = entered

    outputs_buf, scaled_all, weighted_all = buffers
    before_last = mine
    operands = (states[slots - 2], mine, entering, moved[slots - 2], norm_gain, cotan)
    scaled_all, weighted_all = local_call(
        functools.partial(operands_kernel, count),
        stored[1:],
        operands + (scaled_all, weighted_all),
        (),
        {len(operands): 0, len(operands) + 1: 1},
    )
    before = (count - 1) * rows
    (first_sum,) = local_call(
        functools.partial(first_gradient_kernel, rows),
        (jax.ShapeDtypeStruct((cols, width_kv), jnp.float32),),
        (scaled_all, weighted_all),
    )
    outputs_buf = late_emit(states[slots - 2], before_last, swap(before_last, "dp", 1), moved[slots - 2], outputs_buf)
    (mine,) = local_call(
        functools.partial(value_kernel, pairs, cols * dp_count), (message,), waiting + [first_sum, outputs_buf]
    )
    (gradient,) = local_call(
        functools.partial(gradient_kernel, count),
        (bf16(cols, width_kv),),
        (states[slots - 1], mine, entering, moved[slots - 1], norm_gain, cotan[before:], first_sum),
        (),
        None,
        values,
    )

    share = width_kv // dp_count
    right_rows = None
    earlier = ()
    for masks in ((pairs - 1,), tuple(range(pairs - 2, -1, -1))):
        part = bf16(len(masks), share, width_kv)
        ours, theirs = local_call(
            functools.partial(right_kernel, masks),
            (part, part),
            (states[0], gradient) + earlier,
            (),
            None,
            (pltpu.VMEM((2 * share, width_kv), jnp.float32),),
        )
        pieces = local_call(
            right_pieces_kernel,
            tuple(jax.ShapeDtypeStruct((share, width_kv), jnp.bfloat16 if mask else jnp.float32) for mask in masks),
            (ours, swap(theirs, "dp", 1)),
        )
        earlier = tuple(pieces[:1])
        for mask, piece in zip(masks, pieces):
            if mask > 0:
                piece = swap(piece, "dp", 2 * mask)
            piece = piece.astype(jnp.float32)
            right_rows = piece if right_rows is None else right_rows + piece
    right_new = right_old[0] + right_rows / (cols * dp_count)

    outputs_buf = late_emit(states[slots - 1], mine, swap(mine, "dp", 1), moved[slots - 1], outputs_buf)

    order = BLOCK
    height = order // 4
    old_spec = pl.BlockSpec((1, height, order), lambda block, part: (block, part, 0))
    left_new, outputs_buf = pl.pallas_call(
        left_kernel,
        out_shape=(pltpu.HBM(left_old.shape[1:], jnp.float32), pltpu.HBM((tokens, cols), jnp.bfloat16)),
        grid=(cols // order, order // height),
        in_specs=[pl.BlockSpec(memory_space=pltpu.VMEM)] * 2 + [old_spec],
        out_specs=(old_spec, pl.BlockSpec(memory_space=pl.ANY)),
        scratch_shapes=(pltpu.SemaphoreType.DMA,),
        compiler_params=pltpu.CompilerParams(vmem_limit_bytes=16 << 20),
        name="left",
    )(
        pltpu.with_memory_space_constraint(gradient, pltpu.VMEM),
        pltpu.with_memory_space_constraint(outputs_buf, pltpu.VMEM),
        pltpu.with_memory_space_constraint(left_old[0], pltpu.HBM),
    )
    return (outputs_buf.reshape(1, micro_count, rows, cols), left_new[None], right_new[None])


def solution(mesh):
    placed = (
        P(None, None, "dp"),
        P("section", None, None, None),
        P("section", "dp"),
        P("section", "dp", None),
        P("section", None, "dp"),
        P("section", "dp", None, None),
        P("section", "dp", None),
    )
    return jax.shard_map(
        on_device,
        mesh=mesh,
        in_specs=placed,
        out_specs=(
            P("section", None, None, "dp"),
            P("section", "dp", None, None),
            P("section", "dp", None),
        ),
        check_vma=False,
    )
```

```python
import functools

import jax
import jax.numpy as jnp
from jax import lax
from jax.experimental import pallas as pl
from jax.experimental.pallas import tpu as pltpu
from jax.sharding import PartitionSpec as P


BLOCK = 1024
LANES = 128
LAG = 3
EXTRA = 8


def swap(value, axis, mask):
    count = lax.axis_size(axis)
    return lax.ppermute(value, axis, [(i, i ^ mask) for i in range(count)])


def passed_along(value, axis):
    count = lax.axis_size(axis)
    return lax.ppermute(value, axis, [(i, i + 1) for i in range(count - 1)])


def put_pair(ref, total):
    high = total.astype(jnp.bfloat16)
    low = (total - high.astype(jnp.float32)).astype(jnp.bfloat16)
    rows = total.shape[0]
    lane = lax.broadcasted_iota(jnp.int32, (rows, LANES), 1)
    high = jnp.broadcast_to(high.astype(jnp.float32), (rows, LANES))
    low = jnp.broadcast_to(low.astype(jnp.float32), (rows, LANES))
    ref[...] = jnp.where(lane < LANES // 2, high, low).astype(jnp.bfloat16)


def get_pair(block):
    wide = block.astype(jnp.float32)
    return wide[:, :1] + wide[:, LANES // 2 : LANES // 2 + 1]


def project_kernel(count, state_ref, entering_ref, moved_ref, gain_ref, weight_ref, *rest):
    keep_ref, send_ref, next_ref = rest[-3:]
    rows, wide = keep_ref.shape
    half = wide - LANES
    next_ref[0] = state_ref[0]
    next_ref[1] = state_ref[1]
    next_ref[2] = state_ref[2] + 1
    next_ref[3] = state_ref[3]
    hidden = chosen(count, rows, state_ref, entering_ref, moved_ref, slice(None))
    scaled = (hidden * gain_ref[...].astype(jnp.float32)).astype(jnp.bfloat16)
    square = jnp.sum(hidden * hidden, axis=1, keepdims=True)
    put_pair(keep_ref.at[:, half:], square)
    put_pair(send_ref.at[:, half:], square)
    own = pl.multiple_of(state_ref[1] * half, LANES)
    theirs = pl.multiple_of((1 - state_ref[1]) * half, LANES)
    for ref, first_col in ((send_ref, theirs), (keep_ref, own)):
        ref[:, :half] = jnp.dot(
            scaled, weight_ref[:, pl.ds(first_col, half)], preferred_element_type=jnp.float32
        ).astype(jnp.bfloat16)


def chosen(count, rows, state_ref, entering_ref, moved_ref, part):
    first = pl.multiple_of(jnp.minimum(state_ref[2], count - 1) * rows, 16)
    entered = entering_ref[pl.ds(first, rows), part]
    return jnp.where(state_ref[0] == 0, entered, moved_ref[:, part]).astype(jnp.float32)


def place(count, rows, state_ref):
    return pl.ds(pl.multiple_of(jnp.clip(state_ref[2] - LAG * state_ref[0], 0, count - 1) * rows, 16), rows)


def join_kernel(mine_ref, other_ref, out_ref):
    rows = mine_ref.shape[0]
    half = out_ref.shape[1]
    out_ref[:rows, :] = (
        mine_ref[:, :half].astype(jnp.float32) + other_ref[:, :half].astype(jnp.float32)
    ).astype(jnp.bfloat16)
    total = get_pair(mine_ref[:, half:]) + get_pair(other_ref[:, half:])
    along = jnp.transpose(jnp.broadcast_to(total, (rows, LANES)))[:EXTRA, :]
    high = along.astype(jnp.bfloat16)
    out_ref[rows:, :] = jnp.zeros((EXTRA, half), jnp.bfloat16)
    out_ref[rows:, :rows] = high
    out_ref[rows:, rows : 2 * rows] = (along - high.astype(jnp.float32)).astype(jnp.bfloat16)


def value_kernel(pairs, model_width, *refs):
    parts, out_ref = refs[:pairs], refs[-1]
    rows = out_ref.shape[0]
    half = out_ref.shape[1] - LANES
    total = jnp.zeros((rows, half), jnp.float32)
    square = jnp.zeros((EXTRA, rows), jnp.float32)
    for part in parts:
        total += part[:rows, :].astype(jnp.float32)
        square += part[rows:, :rows].astype(jnp.float32) + part[rows:, rows : 2 * rows].astype(jnp.float32)
    inv_rms = lax.rsqrt(square / model_width + 0.25)
    inv_rms = jnp.transpose(jnp.broadcast_to(inv_rms[:1, :], (LANES, rows)))[:, :1]
    out_ref[:, :half] = (inv_rms * total).astype(jnp.bfloat16)
    put_pair(out_ref.at[:, half:], inv_rms)


def gather_values(state_ref, mine_ref, other_ref, values):
    half = mine_ref.shape[1] - LANES
    values[:, pl.ds(pl.multiple_of(state_ref[1] * half, LANES), half)] = mine_ref[:, :half]
    values[:, pl.ds(pl.multiple_of((1 - state_ref[1]) * half, LANES), half)] = other_ref[:, :half]


def keep_operands(count, state_ref, mine_ref, hidden, gain_ref, cotan_ref, scaled_ref, weighted_ref):
    rows, wide = mine_ref.shape
    at = place(count, rows, state_ref)
    scaled_ref[at, :] = (hidden * gain_ref[...].astype(jnp.float32)).astype(jnp.bfloat16)
    inv_rms = get_pair(mine_ref[:, wide - LANES :])
    weighted_ref[at, :] = (inv_rms * cotan_ref[at, :].astype(jnp.float32)).astype(jnp.bfloat16)


def output_kernel(count, state_ref, mine_ref, other_ref, entering_ref, moved_ref, weight_ref, gain_ref, cotan_ref, *rest):
    result_ref, out_ref, scaled_ref, weighted_ref, values = rest[-5:]
    rows = mine_ref.shape[0]
    gather_values(state_ref, mine_ref, other_ref, values)
    at = place(count, rows, state_ref)
    inv_rms = get_pair(mine_ref[:, mine_ref.shape[1] - LANES :])
    weighted_ref[at, :] = (inv_rms * cotan_ref[at, :].astype(jnp.float32)).astype(jnp.bfloat16)
    hidden = chosen(count, rows, state_ref, entering_ref, moved_ref, slice(None))
    scaled_ref[at, :] = (hidden * gain_ref[...].astype(jnp.float32)).astype(jnp.bfloat16)
    result = (hidden + jnp.dot(values[...], weight_ref[...], preferred_element_type=jnp.float32)).astype(jnp.bfloat16)
    result_ref[...] = result
    out_ref[at, :] = result


def operands_kernel(count, state_ref, mine_ref, entering_ref, moved_ref, gain_ref, cotan_ref, *rest):
    scaled_ref, weighted_ref = rest[-2:]
    hidden = chosen(count, mine_ref.shape[0], state_ref, entering_ref, moved_ref, slice(None))
    keep_operands(count, state_ref, mine_ref, hidden, gain_ref, cotan_ref, scaled_ref, weighted_ref)


def late_output_kernel(count, state_ref, mine_ref, other_ref, entering_ref, moved_ref, weight_ref, *rest):
    out_ref, values = rest[-2:]
    rows = mine_ref.shape[0]
    gather_values(state_ref, mine_ref, other_ref, values)
    hidden = chosen(count, rows, state_ref, entering_ref, moved_ref, slice(None))
    out_ref[place(count, rows, state_ref), :] = (
        hidden + jnp.dot(values[...], weight_ref[...], preferred_element_type=jnp.float32)
    ).astype(jnp.bfloat16)


CONTRACT_ROWS = (((0,), (0,)), ((), ()))


def first_gradient_kernel(rows, scaled_ref, weighted_ref, out_ref):
    cols, _ = out_ref.shape
    before = weighted_ref.shape[0] - rows
    tile = min(512, cols)

    @pl.loop(0, cols // tile)
    def _(index):
        at = pl.ds(pl.multiple_of(index * tile, tile), tile)
        out_ref[at, :] = lax.dot_general(
            scaled_ref[:before, at], weighted_ref[:before, :], CONTRACT_ROWS, preferred_element_type=jnp.float32
        )


def gradient_kernel(count, state_ref, mine_ref, entering_ref, moved_ref, gain_ref, cotan_ref, sum_ref, out_ref, weighted):
    rows, wide = mine_ref.shape
    cols = out_ref.shape[0]
    tile = min(512, cols)
    inv_rms = get_pair(mine_ref[:, wide - LANES :])
    weighted[...] = (inv_rms * cotan_ref[...].astype(jnp.float32)).astype(jnp.bfloat16)

    @pl.loop(0, cols // tile)
    def _(index):
        at = pl.ds(pl.multiple_of(index * tile, tile), tile)
        hidden = chosen(count, rows, state_ref, entering_ref, moved_ref, at)
        scaled = (hidden * gain_ref[:, at].astype(jnp.float32)).astype(jnp.bfloat16)
        out_ref[at, :] = (
            sum_ref[at, :]
            + lax.dot_general(scaled, weighted[...], CONTRACT_ROWS, preferred_element_type=jnp.float32)
        ).astype(jnp.bfloat16)


def right_kernel(masks, state_ref, gradient_ref, *rest):
    ours_ref, theirs_ref, block = rest[-3:]
    _, share, _ = ours_ref.shape

    @pl.loop(0, len(masks))
    def _(index):
        pair = state_ref[3] ^ (masks[0] - index)
        at = pl.ds(pl.multiple_of(pair * 2 * share, 2 * share), 2 * share)
        block[...] = lax.dot_general(
            gradient_ref[:, at], gradient_ref[...], CONTRACT_ROWS, preferred_element_type=jnp.float32
        )
        core = state_ref[1]
        ours_ref[index] = block[pl.ds(pl.multiple_of(core * share, share), share), :].astype(jnp.bfloat16)
        theirs_ref[index] = block[pl.ds(pl.multiple_of((1 - core) * share, share), share), :].astype(jnp.bfloat16)


def right_pieces_kernel(pieces, ours_ref, came_ref, *rest):
    for index, ref in enumerate(rest[-pieces:]):
        ref[...] = (ours_ref[index].astype(jnp.float32) + came_ref[index].astype(jnp.float32)).astype(ref.dtype)


def left_kernel(gradient_ref, held_ref, old_ref, out_ref, stored_ref, sem):
    block, part = pl.program_id(0), pl.program_id(1)
    height, order = old_ref.shape[1:]
    store = pltpu.make_async_copy(held_ref, stored_ref, sem)

    @pl.when((block == 0) & (part == 0))
    def _():
        store.start()

    whole = pl.ds(pl.multiple_of(block * order, order), order)
    rows = pl.ds(pl.multiple_of(block * order + part * height, height), height)
    product = lax.dot_general(
        gradient_ref[rows, :], gradient_ref[whole, :], (((1,), (1,)), ((), ())), preferred_element_type=jnp.float32
    )
    out_ref[0] = old_ref[0] + product / order

    @pl.when((block == pl.num_programs(0) - 1) & (part == pl.num_programs(1) - 1))
    def _():
        store.wait()


def local_call(kernel, outs, operands, remote=(), aliases=None, scratch=(), limit=16):
    def space(x):
        return pltpu.SMEM if x.dtype == jnp.int32 else pltpu.VMEM

    far = [o for o in outs if isinstance(o, tuple)]
    near = [o for o in outs if not isinstance(o, tuple)]
    hbm = pl.BlockSpec(memory_space=pl.ANY)
    return pl.pallas_call(
        kernel,
        out_shape=tuple([space(o)(o.shape, o.dtype) for o in near] + [pltpu.HBM(*o) for o in far]),
        in_specs=[pl.BlockSpec(memory_space=space(x)) for x in operands] + [hbm] * len(remote),
        out_specs=tuple([pl.BlockSpec(memory_space=space(o)) for o in near] + [hbm] * len(far)),
        scratch_shapes=scratch,
        input_output_aliases=aliases or {},
        compiler_params=pltpu.CompilerParams(vmem_limit_bytes=limit << 20),
    )(*[pltpu.with_memory_space_constraint(x, space(x)) for x in operands], *remote)


def on_device(inputs, cotangent, norm_gain, value_weight, output_weight, left_old, right_old):
    sections = lax.axis_size("section")
    dp_count = lax.axis_size("dp")
    section_index = lax.axis_index("section")
    owner_index = lax.axis_index("dp")
    core_index = owner_index % 2
    pair_index = owner_index // 2
    pairs = dp_count // 2
    micro_count, rows, cols = inputs.shape
    width_kv = value_weight.shape[2]
    half = width_kv // 2
    wide = half + LANES
    tokens = micro_count * rows
    entering = inputs.reshape(tokens, cols)
    cotan = cotangent.reshape(tokens, width_kv)
    w_value = value_weight[0]
    w_output = output_weight[0]
    state = jnp.stack([section_index, core_index, jnp.zeros_like(core_index), pair_index]).astype(jnp.int32)
    count = micro_count
    slots = count + LAG * (sections - 1)
    bf16 = lambda *shape: jax.ShapeDtypeStruct(shape, jnp.bfloat16)
    message = bf16(rows, wide)

    def project(state, moved, behind):
        alone = behind is None
        return local_call(
            functools.partial(project_kernel, 1 if alone else count),
            (message, message, jax.ShapeDtypeStruct(state.shape, jnp.int32)),
            (state, inputs[0] if alone else entering, moved, norm_gain, w_value) + (() if behind is None else (behind,)),
        )

    stored = (bf16(tokens, cols), bf16(tokens, cols), bf16(tokens, width_kv))
    values = (pltpu.VMEM((rows, width_kv), jnp.bfloat16),)

    def emit(state, mine, other, moved, buffers):
        operands = (state, mine, other, entering, moved, w_output, norm_gain, cotan)
        return local_call(
            functools.partial(output_kernel, count),
            (bf16(rows, cols),) + stored,
            operands + buffers,
            (),
            {len(operands) + i: 1 + i for i in range(len(buffers))},
            values,
        )

    def late_emit(state, mine, other, moved, held, *extra):
        operands = (state, mine, other, entering, moved, w_output)
        (held,) = local_call(
            functools.partial(late_output_kernel, count),
            stored[:1],
            operands + (held,) + extra,
            (),
            {len(operands): 0},
            values,
        )
        return held

    buffers = ()
    moved = [jnp.zeros((rows, cols), jnp.bfloat16)] * LAG
    states = [state]
    waiting = None
    behind = None
    for slot in range(slots):
        keep, send, state = project(states[slot], moved[slot], behind if slot else None)
        states.append(state)
        (pair_sum,) = local_call(join_kernel, (bf16(rows + EXTRA, half),), (keep, swap(send, "dp", 1)))
        entered = [pair_sum]
        for mask in range(pairs - 1, 0, -1):
            entered.append(swap(pair_sum, "dp", 2 * mask))
        if slot == 0:
            behind = pair_sum
        if slot > 0:
            (mine,) = local_call(
                functools.partial(value_kernel, pairs, cols * dp_count), (message,), waiting + [pair_sum]
            )
            if slot < slots - 1:
                behind, *buffers = emit(states[slot - 1], mine, swap(mine, "dp", 1), moved[slot - 1], tuple(buffers))
            if slot - 1 + LAG < slots:
                moved.append(passed_along(behind, "section"))
        waiting = entered

    outputs_buf, scaled_all, weighted_all = buffers
    before_last = mine
    operands = (states[slots - 2], mine, entering, moved[slots - 2], norm_gain, cotan)
    scaled_all, weighted_all = local_call(
        functools.partial(operands_kernel, count),
        stored[1:],
        operands + (scaled_all, weighted_all),
        (),
        {len(operands): 0, len(operands) + 1: 1},
    )
    before = (count - 1) * rows
    (first_sum,) = local_call(
        functools.partial(first_gradient_kernel, rows),
        (jax.ShapeDtypeStruct((cols, width_kv), jnp.float32),),
        (scaled_all, weighted_all),
    )
    outputs_buf = late_emit(states[slots - 2], before_last, swap(before_last, "dp", 1), moved[slots - 2], outputs_buf)
    (mine,) = local_call(
        functools.partial(value_kernel, pairs, cols * dp_count), (message,), waiting + [first_sum, outputs_buf]
    )
    (gradient,) = local_call(
        functools.partial(gradient_kernel, count),
        (bf16(cols, width_kv),),
        (states[slots - 1], mine, entering, moved[slots - 1], norm_gain, cotan[before:], first_sum),
        (),
        None,
        values,
    )

    other = swap(mine, "dp", 1)
    share = width_kv // dp_count
    right_rows = None
    earlier = ()
    for masks in ((pairs - 1,), tuple(range(pairs - 2, -1, -1))):
        part = bf16(len(masks), share, width_kv)
        ours, theirs = local_call(
            functools.partial(right_kernel, masks),
            (part, part),
            (states[0], gradient) + earlier,
            (),
            None,
            (pltpu.VMEM((2 * share, width_kv), jnp.float32),),
        )
        if earlier:
            outputs_buf = late_emit(states[slots - 1], mine, other, moved[slots - 1], outputs_buf, theirs)
        pieces = local_call(
            functools.partial(right_pieces_kernel, len(masks)),
            tuple(jax.ShapeDtypeStruct((share, width_kv), jnp.bfloat16 if mask else jnp.float32) for mask in masks),
            (ours, swap(theirs, "dp", 1)) + ((outputs_buf,) if earlier else ()),
        )
        earlier = tuple(pieces[:1])
        for mask, piece in zip(masks, pieces):
            if mask > 0:
                piece = swap(piece, "dp", 2 * mask)
            piece = piece.astype(jnp.float32)
            right_rows = piece if right_rows is None else right_rows + piece
    right_new = right_old[0] + right_rows / (cols * dp_count)

    order = BLOCK
    height = order // 2
    old_spec = pl.BlockSpec((1, height, order), lambda block, part: (block, part, 0))
    left_new, outputs_buf = pl.pallas_call(
        left_kernel,
        out_shape=(pltpu.HBM(left_old.shape[1:], jnp.float32), pltpu.HBM((tokens, cols), jnp.bfloat16)),
        grid=(cols // order, order // height),
        in_specs=[pl.BlockSpec(memory_space=pltpu.VMEM)] * 2 + [old_spec],
        out_specs=(old_spec, pl.BlockSpec(memory_space=pl.ANY)),
        scratch_shapes=(pltpu.SemaphoreType.DMA,),
        compiler_params=pltpu.CompilerParams(vmem_limit_bytes=20 << 20),
        name="left",
    )(
        pltpu.with_memory_space_constraint(gradient, pltpu.VMEM),
        pltpu.with_memory_space_constraint(outputs_buf, pltpu.VMEM),
        pltpu.with_memory_space_constraint(left_old[0], pltpu.HBM),
    )
    return (outputs_buf.reshape(1, micro_count, rows, cols), left_new[None], right_new[None])


def solution(mesh):
    placed = (
        P(None, None, "dp"),
        P("section", None, None, None),
        P("section", "dp"),
        P("section", "dp", None),
        P("section", None, "dp"),
        P("section", "dp", None, None),
        P("section", "dp", None),
    )
    return jax.shard_map(
        on_device,
        mesh=mesh,
        in_specs=placed,
        out_specs=(
            P("section", None, None, "dp"),
            P("section", "dp", None, None),
            P("section", "dp", None),
        ),
        check_vma=False,
    )
```

```python
import functools

import jax
import jax.numpy as jnp
from jax import lax
from jax.experimental import pallas as pl
from jax.experimental.pallas import tpu as pltpu
from jax.sharding import PartitionSpec as P


BLOCK = 1024
LANES = 128
LAG = 3
EXTRA = 8


def swap(value, axis, mask):
    count = lax.axis_size(axis)
    return lax.ppermute(value, axis, [(i, i ^ mask) for i in range(count)])


def passed_along(value, axis):
    count = lax.axis_size(axis)
    return lax.ppermute(value, axis, [(i, i + 1) for i in range(count - 1)])


def put_pair(ref, total):
    high = total.astype(jnp.bfloat16)
    low = (total - high.astype(jnp.float32)).astype(jnp.bfloat16)
    rows = total.shape[0]
    lane = lax.broadcasted_iota(jnp.int32, (rows, LANES), 1)
    high = jnp.broadcast_to(high.astype(jnp.float32), (rows, LANES))
    low = jnp.broadcast_to(low.astype(jnp.float32), (rows, LANES))
    ref[...] = jnp.where(lane < LANES // 2, high, low).astype(jnp.bfloat16)


def get_pair(block):
    wide = block.astype(jnp.float32)
    return wide[:, :1] + wide[:, LANES // 2 : LANES // 2 + 1]


def project_kernel(count, state_ref, entering_ref, moved_ref, gain_ref, weight_ref, *rest):
    send_ref, scaled_ref, next_ref = rest[-3:]
    rows, wide = send_ref.shape
    half = wide - LANES
    next_ref[0] = state_ref[0]
    next_ref[1] = state_ref[1]
    next_ref[2] = state_ref[2] + 1
    next_ref[3] = state_ref[3]
    hidden = chosen(count, rows, state_ref, entering_ref, moved_ref, slice(None))
    scaled = (hidden * gain_ref[...].astype(jnp.float32)).astype(jnp.bfloat16)
    scaled_ref[...] = scaled
    put_pair(send_ref.at[:, half:], jnp.sum(hidden * hidden, axis=1, keepdims=True))
    theirs = pl.multiple_of((1 - state_ref[1]) * half, LANES)
    send_ref[:, :half] = jnp.dot(
        scaled, weight_ref[:, pl.ds(theirs, half)], preferred_element_type=jnp.float32
    ).astype(jnp.bfloat16)


def keep_kernel(state_ref, scaled_ref, weight_ref, keep_ref):
    half = keep_ref.shape[1]
    own = pl.multiple_of(state_ref[1] * half, LANES)
    keep_ref[...] = jnp.dot(
        scaled_ref[...], weight_ref[:, pl.ds(own, half)], preferred_element_type=jnp.float32
    ).astype(jnp.bfloat16)


def chosen(count, rows, state_ref, entering_ref, moved_ref, part):
    first = pl.multiple_of(jnp.minimum(state_ref[2], count - 1) * rows, 16)
    entered = entering_ref[pl.ds(first, rows), part]
    return jnp.where(state_ref[0] == 0, entered, moved_ref[:, part]).astype(jnp.float32)


def place(count, rows, state_ref):
    return pl.ds(pl.multiple_of(jnp.clip(state_ref[2] - LAG * state_ref[0], 0, count - 1) * rows, 16), rows)


def join_kernel(mine_ref, sent_ref, other_ref, out_ref):
    rows = mine_ref.shape[0]
    half = out_ref.shape[1]
    out_ref[:rows, :] = (
        mine_ref[:, :half].astype(jnp.float32) + other_ref[:, :half].astype(jnp.float32)
    ).astype(jnp.bfloat16)
    total = get_pair(sent_ref[:, half:]) + get_pair(other_ref[:, half:])
    along = jnp.transpose(jnp.broadcast_to(total, (rows, LANES)))[:EXTRA, :]
    high = along.astype(jnp.bfloat16)
    out_ref[rows:, :] = jnp.zeros((EXTRA, half), jnp.bfloat16)
    out_ref[rows:, :rows] = high
    out_ref[rows:, rows : 2 * rows] = (along - high.astype(jnp.float32)).astype(jnp.bfloat16)


def value_kernel(pairs, model_width, *refs):
    parts, out_ref = refs[:pairs], refs[-1]
    rows = out_ref.shape[0]
    half = out_ref.shape[1] - LANES
    total = jnp.zeros((rows, half), jnp.float32)
    square = jnp.zeros((EXTRA, rows), jnp.float32)
    for part in parts:
        total += part[:rows, :].astype(jnp.float32)
        square += part[rows:, :rows].astype(jnp.float32) + part[rows:, rows : 2 * rows].astype(jnp.float32)
    inv_rms = lax.rsqrt(square / model_width + 0.25)
    inv_rms = jnp.transpose(jnp.broadcast_to(inv_rms[:1, :], (LANES, rows)))[:, :1]
    out_ref[:, :half] = (inv_rms * total).astype(jnp.bfloat16)
    put_pair(out_ref.at[:, half:], inv_rms)


def gather_values(state_ref, mine_ref, other_ref, values):
    half = mine_ref.shape[1] - LANES
    values[:, pl.ds(pl.multiple_of(state_ref[1] * half, LANES), half)] = mine_ref[:, :half]
    values[:, pl.ds(pl.multiple_of((1 - state_ref[1]) * half, LANES), half)] = other_ref[:, :half]


def keep_operands(count, state_ref, mine_ref, hidden, gain_ref, cotan_ref, scaled_ref, weighted_ref):
    rows, wide = mine_ref.shape
    at = place(count, rows, state_ref)
    scaled_ref[at, :] = (hidden * gain_ref[...].astype(jnp.float32)).astype(jnp.bfloat16)
    inv_rms = get_pair(mine_ref[:, wide - LANES :])
    weighted_ref[at, :] = (inv_rms * cotan_ref[at, :].astype(jnp.float32)).astype(jnp.bfloat16)


def output_kernel(count, state_ref, mine_ref, other_ref, entering_ref, moved_ref, weight_ref, gain_ref, cotan_ref, *rest):
    result_ref, out_ref, scaled_ref, weighted_ref, values = rest[-5:]
    rows = mine_ref.shape[0]
    gather_values(state_ref, mine_ref, other_ref, values)
    at = place(count, rows, state_ref)
    inv_rms = get_pair(mine_ref[:, mine_ref.shape[1] - LANES :])
    weighted_ref[at, :] = (inv_rms * cotan_ref[at, :].astype(jnp.float32)).astype(jnp.bfloat16)
    hidden = chosen(count, rows, state_ref, entering_ref, moved_ref, slice(None))
    scaled_ref[at, :] = (hidden * gain_ref[...].astype(jnp.float32)).astype(jnp.bfloat16)
    result = (hidden + jnp.dot(values[...], weight_ref[...], preferred_element_type=jnp.float32)).astype(jnp.bfloat16)
    result_ref[...] = result
    out_ref[at, :] = result


def operands_kernel(count, state_ref, mine_ref, entering_ref, moved_ref, gain_ref, cotan_ref, *rest):
    scaled_ref, weighted_ref = rest[-2:]
    hidden = chosen(count, mine_ref.shape[0], state_ref, entering_ref, moved_ref, slice(None))
    keep_operands(count, state_ref, mine_ref, hidden, gain_ref, cotan_ref, scaled_ref, weighted_ref)


def late_output_kernel(count, state_ref, mine_ref, other_ref, entering_ref, moved_ref, weight_ref, *rest):
    out_ref, values = rest[-2:]
    rows = mine_ref.shape[0]
    gather_values(state_ref, mine_ref, other_ref, values)
    hidden = chosen(count, rows, state_ref, entering_ref, moved_ref, slice(None))
    out_ref[place(count, rows, state_ref), :] = (
        hidden + jnp.dot(values[...], weight_ref[...], preferred_element_type=jnp.float32)
    ).astype(jnp.bfloat16)


CONTRACT_ROWS = (((0,), (0,)), ((), ()))


def first_gradient_kernel(rows, scaled_ref, weighted_ref, out_ref):
    cols, _ = out_ref.shape
    before = weighted_ref.shape[0] - rows
    tile = min(512, cols)

    @pl.loop(0, cols // tile)
    def _(index):
        at = pl.ds(pl.multiple_of(index * tile, tile), tile)
        out_ref[at, :] = lax.dot_general(
            scaled_ref[:before, at], weighted_ref[:before, :], CONTRACT_ROWS, preferred_element_type=jnp.float32
        )


def gradient_kernel(count, state_ref, mine_ref, entering_ref, moved_ref, gain_ref, cotan_ref, sum_ref, out_ref, weighted):
    rows, wide = mine_ref.shape
    cols = out_ref.shape[0]
    tile = min(512, cols)
    inv_rms = get_pair(mine_ref[:, wide - LANES :])
    weighted[...] = (inv_rms * cotan_ref[...].astype(jnp.float32)).astype(jnp.bfloat16)

    @pl.loop(0, cols // tile)
    def _(index):
        at = pl.ds(pl.multiple_of(index * tile, tile), tile)
        hidden = chosen(count, rows, state_ref, entering_ref, moved_ref, at)
        scaled = (hidden * gain_ref[:, at].astype(jnp.float32)).astype(jnp.bfloat16)
        out_ref[at, :] = (
            sum_ref[at, :]
            + lax.dot_general(scaled, weighted[...], CONTRACT_ROWS, preferred_element_type=jnp.float32)
        ).astype(jnp.bfloat16)


def right_kernel(masks, state_ref, gradient_ref, *rest):
    ours_ref, theirs_ref, block = rest[-3:]
    _, share, _ = ours_ref.shape

    @pl.loop(0, len(masks))
    def _(index):
        pair = state_ref[3] ^ (masks[0] - index)
        at = pl.ds(pl.multiple_of(pair * 2 * share, 2 * share), 2 * share)
        block[...] = lax.dot_general(
            gradient_ref[:, at], gradient_ref[...], CONTRACT_ROWS, preferred_element_type=jnp.float32
        )
        core = state_ref[1]
        ours_ref[index] = block[pl.ds(pl.multiple_of(core * share, share), share), :].astype(jnp.bfloat16)
        theirs_ref[index] = block[pl.ds(pl.multiple_of((1 - core) * share, share), share), :].astype(jnp.bfloat16)


def right_pieces_kernel(pieces, ours_ref, came_ref, *rest):
    for index, ref in enumerate(rest[-pieces:]):
        ref[...] = (ours_ref[index].astype(jnp.float32) + came_ref[index].astype(jnp.float32)).astype(ref.dtype)


def left_kernel(gradient_ref, held_ref, old_ref, out_ref, stored_ref, sem):
    block, part = pl.program_id(0), pl.program_id(1)
    height, order = old_ref.shape[1:]
    store = pltpu.make_async_copy(held_ref, stored_ref, sem)

    @pl.when((block == 0) & (part == 0))
    def _():
        store.start()

    whole = pl.ds(pl.multiple_of(block * order, order), order)
    rows = pl.ds(pl.multiple_of(block * order + part * height, height), height)
    product = lax.dot_general(
        gradient_ref[rows, :], gradient_ref[whole, :], (((1,), (1,)), ((), ())), preferred_element_type=jnp.float32
    )
    out_ref[0] = old_ref[0] + product / order

    @pl.when((block == pl.num_programs(0) - 1) & (part == pl.num_programs(1) - 1))
    def _():
        store.wait()


def local_call(kernel, outs, operands, remote=(), aliases=None, scratch=(), limit=16):
    def space(x):
        return pltpu.SMEM if x.dtype == jnp.int32 else pltpu.VMEM

    far = [o for o in outs if isinstance(o, tuple)]
    near = [o for o in outs if not isinstance(o, tuple)]
    hbm = pl.BlockSpec(memory_space=pl.ANY)
    return pl.pallas_call(
        kernel,
        out_shape=tuple([space(o)(o.shape, o.dtype) for o in near] + [pltpu.HBM(*o) for o in far]),
        in_specs=[pl.BlockSpec(memory_space=space(x)) for x in operands] + [hbm] * len(remote),
        out_specs=tuple([pl.BlockSpec(memory_space=space(o)) for o in near] + [hbm] * len(far)),
        scratch_shapes=scratch,
        input_output_aliases=aliases or {},
        compiler_params=pltpu.CompilerParams(vmem_limit_bytes=limit << 20),
    )(*[pltpu.with_memory_space_constraint(x, space(x)) for x in operands], *remote)


def on_device(inputs, cotangent, norm_gain, value_weight, output_weight, left_old, right_old):
    sections = lax.axis_size("section")
    dp_count = lax.axis_size("dp")
    section_index = lax.axis_index("section")
    owner_index = lax.axis_index("dp")
    core_index = owner_index % 2
    pair_index = owner_index // 2
    pairs = dp_count // 2
    micro_count, rows, cols = inputs.shape
    width_kv = value_weight.shape[2]
    half = width_kv // 2
    wide = half + LANES
    tokens = micro_count * rows
    entering = inputs.reshape(tokens, cols)
    cotan = cotangent.reshape(tokens, width_kv)
    w_value = value_weight[0]
    w_output = output_weight[0]
    state = jnp.stack([section_index, core_index, jnp.zeros_like(core_index), pair_index]).astype(jnp.int32)
    count = micro_count
    slots = count + LAG * (sections - 1)
    bf16 = lambda *shape: jax.ShapeDtypeStruct(shape, jnp.bfloat16)
    message = bf16(rows, wide)

    def project(state, moved, behind):
        alone = behind is None
        return local_call(
            functools.partial(project_kernel, 1 if alone else count),
            (message, bf16(rows, cols), jax.ShapeDtypeStruct(state.shape, jnp.int32)),
            (state, inputs[0] if alone else entering, moved, norm_gain, w_value) + (() if behind is None else (behind,)),
        )

    stored = (bf16(tokens, cols), bf16(tokens, cols), bf16(tokens, width_kv))
    values = (pltpu.VMEM((rows, width_kv), jnp.bfloat16),)

    def emit(state, mine, other, moved, buffers):
        operands = (state, mine, other, entering, moved, w_output, norm_gain, cotan)
        return local_call(
            functools.partial(output_kernel, count),
            (bf16(rows, cols),) + stored,
            operands + buffers,
            (),
            {len(operands) + i: 1 + i for i in range(len(buffers))},
            values,
        )

    def late_emit(state, mine, other, moved, held, *extra):
        operands = (state, mine, other, entering, moved, w_output)
        (held,) = local_call(
            functools.partial(late_output_kernel, count),
            stored[:1],
            operands + (held,) + extra,
            (),
            {len(operands): 0},
            values,
        )
        return held

    buffers = ()
    moved = [jnp.zeros((rows, cols), jnp.bfloat16)] * LAG
    states = [state]
    waiting = None
    behind = None
    for slot in range(slots):
        send, scaled, state = project(states[slot], moved[slot], behind if slot else None)
        came = swap(send, "dp", 1)
        (keep,) = local_call(keep_kernel, (bf16(rows, half),), (states[slot], scaled, w_value))
        states.append(state)
        (pair_sum,) = local_call(join_kernel, (bf16(rows + EXTRA, half),), (keep, send, came))
        entered = [pair_sum]
        for mask in range(pairs - 1, 0, -1):
            entered.append(swap(pair_sum, "dp", 2 * mask))
        if slot == 0:
            behind = pair_sum
        if slot > 0:
            (mine,) = local_call(
                functools.partial(value_kernel, pairs, cols * dp_count), (message,), waiting + [pair_sum]
            )
            if slot < slots - 1:
                behind, *buffers = emit(states[slot - 1], mine, swap(mine, "dp", 1), moved[slot - 1], tuple(buffers))
            if slot - 1 + LAG < slots:
                moved.append(passed_along(behind, "section"))
        waiting = entered

    outputs_buf, scaled_all, weighted_all = buffers
    before_last = mine
    operands = (states[slots - 2], mine, entering, moved[slots - 2], norm_gain, cotan)
    scaled_all, weighted_all = local_call(
        functools.partial(operands_kernel, count),
        stored[1:],
        operands + (scaled_all, weighted_all),
        (),
        {len(operands): 0, len(operands) + 1: 1},
    )
    before = (count - 1) * rows
    (first_sum,) = local_call(
        functools.partial(first_gradient_kernel, rows),
        (jax.ShapeDtypeStruct((cols, width_kv), jnp.float32),),
        (scaled_all, weighted_all),
    )
    outputs_buf = late_emit(states[slots - 2], before_last, swap(before_last, "dp", 1), moved[slots - 2], outputs_buf)
    (mine,) = local_call(
        functools.partial(value_kernel, pairs, cols * dp_count), (message,), waiting + [first_sum, outputs_buf]
    )
    (gradient,) = local_call(
        functools.partial(gradient_kernel, count),
        (bf16(cols, width_kv),),
        (states[slots - 1], mine, entering, moved[slots - 1], norm_gain, cotan[before:], first_sum),
        (),
        None,
        values,
    )

    other = swap(mine, "dp", 1)
    share = width_kv // dp_count
    right_rows = None
    earlier = ()
    for masks in ((pairs - 1,), tuple(range(pairs - 2, -1, -1))):
        part = bf16(len(masks), share, width_kv)
        ours, theirs = local_call(
            functools.partial(right_kernel, masks),
            (part, part),
            (states[0], gradient) + earlier,
            (),
            None,
            (pltpu.VMEM((2 * share, width_kv), jnp.float32),),
        )
        if earlier:
            outputs_buf = late_emit(states[slots - 1], mine, other, moved[slots - 1], outputs_buf, theirs)
        pieces = local_call(
            functools.partial(right_pieces_kernel, len(masks)),
            tuple(jax.ShapeDtypeStruct((share, width_kv), jnp.bfloat16 if mask else jnp.float32) for mask in masks),
            (ours, swap(theirs, "dp", 1)) + ((outputs_buf,) if earlier else ()),
        )
        earlier = tuple(pieces[:1])
        for mask, piece in zip(masks, pieces):
            if mask > 0:
                piece = swap(piece, "dp", 2 * mask)
            piece = piece.astype(jnp.float32)
            right_rows = piece if right_rows is None else right_rows + piece
    right_new = right_old[0] + right_rows / (cols * dp_count)

    order = BLOCK
    height = order // 2
    old_spec = pl.BlockSpec((1, height, order), lambda block, part: (block, part, 0))
    left_new, outputs_buf = pl.pallas_call(
        left_kernel,
        out_shape=(pltpu.HBM(left_old.shape[1:], jnp.float32), pltpu.HBM((tokens, cols), jnp.bfloat16)),
        grid=(cols // order, order // height),
        in_specs=[pl.BlockSpec(memory_space=pltpu.VMEM)] * 2 + [old_spec],
        out_specs=(old_spec, pl.BlockSpec(memory_space=pl.ANY)),
        scratch_shapes=(pltpu.SemaphoreType.DMA,),
        compiler_params=pltpu.CompilerParams(vmem_limit_bytes=20 << 20),
        name="left",
    )(
        pltpu.with_memory_space_constraint(gradient, pltpu.VMEM),
        pltpu.with_memory_space_constraint(outputs_buf, pltpu.VMEM),
        pltpu.with_memory_space_constraint(left_old[0], pltpu.HBM),
    )
    return (outputs_buf.reshape(1, micro_count, rows, cols), left_new[None], right_new[None])


def solution(mesh):
    placed = (
        P(None, None, "dp"),
        P("section", None, None, None),
        P("section", "dp"),
        P("section", "dp", None),
        P("section", None, "dp"),
        P("section", "dp", None, None),
        P("section", "dp", None),
    )
    return jax.shard_map(
        on_device,
        mesh=mesh,
        in_specs=placed,
        out_specs=(
            P("section", None, None, "dp"),
            P("section", "dp", None, None),
            P("section", "dp", None),
        ),
        check_vma=False,
    )
```
